8 devices in a mesh: ep: 8 (over z, y, x, core).
Axes of the slice: x: 2, y: 2, z: 1, core: 2. Of those that a mesh axis runs over, the one named last changes fastest.
Arguments:
- hidden: bfloat16 [16384, 4096], P('ep')
- grad_out: bfloat16 [16384, 4096], P('ep')
- w_router: bfloat16 [4096, 8], replicated
- b_router: float32 [8], replicated
- expert_ids: int32 [16384, 2], P('ep')
- slot_ids: int32 [16384, 2], P('ep')
- w_gate_up: bfloat16 [8, 4096, 2752], P('ep')
- b_gate_up: float32 [8, 2752], P('ep')
- w_down: bfloat16 [8, 1376, 4096], P('ep')
- b_down: float32 [8, 4096], P('ep')
Outputs:
- output 1: bfloat16 [16384, 4096], P('ep')
- output 2: bfloat16 [16384, 4096], P('ep')
- output 3: float32 [4096, 8], replicated
- output 4: float32 [8], replicated
- output 5: float32 [8, 4096, 2752], P('ep')
- output 6: float32 [8, 2752], P('ep')
- output 7: float32 [8, 1376, 4096], P('ep')
- output 8: float32 [8, 4096], P('ep')
All inputs are finite; a program needn't handle non-finite values.
Results may differ from the reference program's by a relative error of at most 0.00836544.
Values are sent between devices in bfloat16 or wider.
A program may use at most 1 GiB of HBM per device.

```python
import jax
import jax.numpy as jnp
from jax import lax

D_MODEL = 4096
FF_EXPERT = 1376
EXPERTS = 8
TOP_K = 2
TOKENS_DEV = 2048
EP_DEVICES = 8

TOKENS = EP_DEVICES * TOKENS_DEV
CAPACITY = (3 * TOKENS_DEV * TOP_K + 2 * EXPERTS - 1) // (2 * EXPERTS)
ROWS_EXPERT = EP_DEVICES * CAPACITY
SWIGLU_LIMIT = 7.0
SWIGLU_ALPHA = 1.702


def draw_routing(key):
    key_bias, key_dev = jax.random.split(key)
    expert_bias = jax.random.randint(key_bias, (EXPERTS,), 0, 512)
    expert_range = jnp.arange(EXPERTS, dtype=jnp.int32)
    copies = TOKENS_DEV * TOP_K

    def one_device(dev_key):
        key_noise, key_hot, key_pick, key_prio = jax.random.split(dev_key, 4)
        noise_int = jax.random.randint(key_noise, (TOKENS_DEV, EXPERTS), 0, 1024)
        hot_expert = jax.random.randint(key_hot, (), 0, EXPERTS)
        forced = jax.random.permutation(key_pick, TOKENS_DEV) < 2 * CAPACITY
        hot_bonus = jnp.where(forced[:, None] & (expert_range[None, :] == hot_expert), 4096, 0)
        scores = (noise_int + expert_bias[None, :] + hot_bonus) * EXPERTS + expert_range[None, :]
        choice = lax.top_k(scores, TOP_K)[1].astype(jnp.int32)
        flat_ids = choice.reshape(-1)
        priority = jax.random.permutation(key_prio, copies)
        sort_order = jnp.argsort(flat_ids * copies + priority)
        counts = jnp.bincount(flat_ids, length=EXPERTS)
        starts = jnp.cumsum(counts) - counts
        rank_sorted = (jnp.arange(copies, dtype=jnp.int32) - starts[flat_ids[sort_order]]).astype(jnp.int32)
        slot_rank = jnp.zeros((copies,), jnp.int32).at[sort_order].set(rank_sorted)
        slot_ids = jnp.where(slot_rank < CAPACITY, slot_rank, -1).reshape(TOKENS_DEV, TOP_K)
        return choice, slot_ids

    choice, slot_ids = jax.vmap(one_device)(jax.random.split(key_dev, EP_DEVICES))
    return choice.reshape(TOKENS, TOP_K), slot_ids.reshape(TOKENS, TOP_K).astype(jnp.int32)


def setup_inputs(seed: int = 0) -> dict:
    key_list = jax.random.split(jax.random.key(seed), 9)
    hidden = jax.random.normal(key_list[0], (TOKENS, D_MODEL), jnp.float32).astype(jnp.bfloat16)
    grad_out = jax.random.normal(key_list[1], (TOKENS, D_MODEL), jnp.float32).astype(jnp.bfloat16)
    w_router = (2.0 * D_MODEL ** -0.5 * jax.random.normal(key_list[2], (D_MODEL, EXPERTS), jnp.float32)).astype(jnp.bfloat16)
    b_router = jax.random.normal(key_list[3], (EXPERTS,), jnp.float32)
    expert_ids, slot_ids = draw_routing(key_list[4])
    w_gate_up = (3.0 * D_MODEL ** -0.5 * jax.random.normal(key_list[5], (EXPERTS, D_MODEL, 2 * FF_EXPERT), jnp.float32)).astype(jnp.bfloat16)
    b_gate_up = jax.random.normal(key_list[6], (EXPERTS, 2 * FF_EXPERT), jnp.float32)
    w_down = (0.15 * FF_EXPERT ** -0.5 * jax.random.normal(key_list[7], (EXPERTS, FF_EXPERT, D_MODEL), jnp.float32)).astype(jnp.bfloat16)
    b_down = 0.5 * jax.random.normal(key_list[8], (EXPERTS, D_MODEL), jnp.float32)
    return {'hidden': hidden, 'grad_out': grad_out, 'w_router': w_router, 'b_router': b_router, 'expert_ids': expert_ids, 'slot_ids': slot_ids, 'w_gate_up': w_gate_up, 'b_gate_up': b_gate_up, 'w_down': w_down, 'b_down': b_down}


def swiglu(pre_act):
    col_pairs = pre_act.reshape(pre_act.shape[:-1] + (pre_act.shape[-1] // 2, 2))
    gate_in = jnp.minimum(col_pairs[..., 0], SWIGLU_LIMIT)
    up_in = jnp.clip(col_pairs[..., 1], -SWIGLU_LIMIT, SWIGLU_LIMIT)
    return gate_in * jax.nn.sigmoid(SWIGLU_ALPHA * gate_in) * (up_in + 1.0)


def reference(hidden, grad_out, w_router, b_router, expert_ids, slot_ids, w_gate_up, b_gate_up, w_down, b_down):
    buf_total = EXPERTS * ROWS_EXPERT
    copy_count = TOKENS * TOP_K
    src_dev = (jnp.arange(TOKENS, dtype=jnp.int32) // TOKENS_DEV)[:, None]
    dest_row = jnp.where(slot_ids >= 0, expert_ids * ROWS_EXPERT + src_dev * CAPACITY + slot_ids, buf_total)
    src_copy = jnp.full((buf_total + 1,), copy_count, jnp.int32).at[dest_row.reshape(-1)].set(jnp.arange(copy_count, dtype=jnp.int32))[:buf_total].reshape(EXPERTS, ROWS_EXPERT)
    logits = jnp.dot(hidden, w_router, preferred_element_type=jnp.float32) + b_router
    gate_w = jax.nn.softmax(jnp.take_along_axis(logits, expert_ids, axis=1), axis=-1)
    flat_gate = gate_w.reshape(-1)

    def expert_forward(expert_args):
        w_gu, b_gu, w_dn, b_dn, src_rows = expert_args
        x_rows = jnp.take(hidden, src_rows // TOP_K, axis=0, mode='fill', fill_value=0)
        pre_act = jnp.dot(x_rows, w_gu, preferred_element_type=jnp.float32) + b_gu
        act_bf = swiglu(pre_act).astype(jnp.bfloat16)
        return (jnp.dot(act_bf, w_dn, preferred_element_type=jnp.float32) + b_dn).astype(jnp.bfloat16)

    y_flat = lax.map(expert_forward, (w_gate_up, b_gate_up, w_down, b_down, src_copy)).reshape(buf_total, D_MODEL)

    def token_forward(block_args):
        gate_blk, dest_blk, grad_blk = block_args
        y_blk = jnp.take(y_flat, dest_blk, axis=0, mode='fill', fill_value=0).astype(jnp.float32)
        out_blk = jnp.sum(gate_blk[:, :, None] * y_blk, axis=1).astype(jnp.bfloat16)
        return out_blk, jnp.einsum('td,tkd->tk', grad_blk.astype(jnp.float32), y_blk)

    dev_shape = (EP_DEVICES, TOKENS_DEV)
    block_out, gate_grad = lax.map(token_forward, (gate_w.reshape(dev_shape + (TOP_K,)), dest_row.reshape(dev_shape + (TOP_K,)), grad_out.reshape(dev_shape + (D_MODEL,))))
    block_out = block_out.reshape(TOKENS, D_MODEL)
    gate_grad = gate_grad.reshape(TOKENS, TOP_K)
    sel_grad = gate_w * (gate_grad - jnp.sum(gate_w * gate_grad, axis=1, keepdims=True))
    logit_grad = jnp.zeros((TOKENS, EXPERTS), jnp.float32).at[jnp.arange(TOKENS)[:, None], expert_ids].add(sel_grad).astype(jnp.bfloat16)

    def expert_backward(expert_args):
        w_gu, b_gu, w_dn, src_rows = expert_args
        tok_rows = src_rows // TOP_K
        x_rows = jnp.take(hidden, tok_rows, axis=0, mode='fill', fill_value=0)
        pre_act = jnp.dot(x_rows, w_gu, preferred_element_type=jnp.float32) + b_gu
        act_val, act_vjp = jax.vjp(swiglu, pre_act)
        act_bf = act_val.astype(jnp.bfloat16)
        row_gate = jnp.take(flat_gate, src_rows, axis=0, mode='fill', fill_value=0)
        row_grad = jnp.take(grad_out, tok_rows, axis=0, mode='fill', fill_value=0).astype(jnp.float32)
        q_rows = (row_gate[:, None] * row_grad).astype(jnp.bfloat16)
        grad_b_dn = jnp.sum(q_rows.astype(jnp.float32), axis=0)
        grad_w_dn = jnp.dot(act_bf.T, q_rows, preferred_element_type=jnp.float32)
        act_grad = jnp.dot(q_rows, w_dn.T, preferred_element_type=jnp.float32)
        pre_grad = act_vjp(act_grad)[0].astype(jnp.bfloat16)
        grad_b_gu = jnp.sum(pre_grad.astype(jnp.float32), axis=0)
        grad_w_gu = jnp.dot(x_rows.T, pre_grad, preferred_element_type=jnp.float32)
        p_rows = jnp.dot(pre_grad, w_gu.T, preferred_element_type=jnp.float32).astype(jnp.bfloat16)
        return grad_w_gu, grad_b_gu, grad_w_dn, grad_b_dn, p_rows

    grad_w_gate_up, grad_b_gate_up, grad_w_down, grad_b_down, p_rows = lax.map(expert_backward, (w_gate_up, b_gate_up, w_down, src_copy))
    p_flat = p_rows.reshape(buf_total, D_MODEL)

    def token_backward(block_args):
        dest_blk, logit_blk = block_args
        p_blk = jnp.take(p_flat, dest_blk, axis=0, mode='fill', fill_value=0).astype(jnp.float32)
        router_dx = jnp.dot(logit_blk, w_router.T, preferred_element_type=jnp.float32)
        return (jnp.sum(p_blk, axis=1) + router_dx).astype(jnp.bfloat16)

    grad_hidden = lax.map(token_backward, (dest_row.reshape(dev_shape + (TOP_K,)), logit_grad.reshape(dev_shape + (EXPERTS,)))).reshape(TOKENS, D_MODEL)
    grad_w_router = jnp.dot(hidden.T, logit_grad, preferred_element_type=jnp.float32)
    grad_b_router = jnp.sum(logit_grad.astype(jnp.float32), axis=0)
    return (block_out, grad_hidden, grad_w_router, grad_b_router, grad_w_gate_up, grad_b_gate_up, grad_w_down, grad_b_down)
```

```python
import jax
import jax.numpy as jnp
from jax import lax
from jax.experimental import pallas as pl
from jax.sharding import PartitionSpec as P

SWIGLU_LIMIT = 7.0
SWIGLU_ALPHA = 1.702
F32 = jnp.float32
BF16 = jnp.bfloat16
ROWS_FIRST = (((0,), (0,)), ((), ()))
COLS_LAST = (((1,), (1,)), ((), ()))


def swiglu(gate, up):
    gate_in = jnp.minimum(gate, SWIGLU_LIMIT)
    up_in = jnp.clip(up, -SWIGLU_LIMIT, SWIGLU_LIMIT)
    return gate_in * jax.nn.sigmoid(SWIGLU_ALPHA * gate_in) * (up_in + 1.0)


def round_up(value, unit):
    return (value + unit - 1) // unit * unit


def add_copies_kernel(first_ref, second_ref, keep_ref, logit_ref, router_ref, *refs):
    out_ref = refs[-1]
    keep = keep_ref[...]
    total = jnp.where(keep[:, 0:1] > 0, first_ref[...].astype(F32), 0.0) + jnp.where(keep[:, 1:2] > 0, second_ref[...].astype(F32), 0.0)
    total += jnp.dot(logit_ref[...], router_ref[...], preferred_element_type=F32)
    out_ref[...] = total.astype(BF16)


def add_copies(first, second, keep, logit_grad, router_t, lo, into):
    rows, cols = first.shape
    d_model = router_t.shape[1]
    experts = router_t.shape[0]
    tm, tn = min(rows, 512), min(cols, 1024)
    base = lo // tn
    args = [first, second, keep, logit_grad, router_t]
    specs = [
        pl.BlockSpec((tm, tn), lambda i, j: (i, j)),
        pl.BlockSpec((tm, tn), lambda i, j: (i, j)),
        pl.BlockSpec((tm, 2), lambda i, j: (i, 0)),
        pl.BlockSpec((tm, experts), lambda i, j: (i, 0)),
        pl.BlockSpec((experts, tn), lambda i, j: (0, j + base)),
    ]
    aliases = {}
    if into is not None:
        args.append(into)
        specs.append(pl.BlockSpec(memory_space=pl.ANY))
        aliases = {5: 0}
    return pl.pallas_call(
        add_copies_kernel,
        out_shape=jax.ShapeDtypeStruct((rows, d_model), BF16),
        grid=(rows // tm, cols // tn),
        in_specs=specs,
        out_specs=pl.BlockSpec((tm, tn), lambda i, j: (i, j + base)),
        input_output_aliases=aliases,
        cost_estimate=pl.CostEstimate(flops=20 * rows * cols, bytes_accessed=6 * rows * cols, transcendentals=0),
    )(*args)


def solution(mesh):
    def block(hidden, grad_out, w_router, b_router, expert_ids, slot_ids, w_gate_up, b_gate_up, w_down, b_down):
        tok_local, d_model = hidden.shape
        top_k = expert_ids.shape[1]
        experts = w_router.shape[1]
        ff2 = w_gate_up.shape[2]
        ff = ff2 // 2
        ffp = round_up(ff, 128)
        capacity = (3 * tok_local * top_k + 2 * experts - 1) // (2 * experts)
        buf_rows = experts * capacity
        copy_count = tok_local * top_k
        x_cuts = (0, round_up(capacity // 6, 8), capacity)
        p_cuts = (0, d_model * 3 // 4, d_model)

        kept = slot_ids >= 0
        dest_row = jnp.where(kept, expert_ids * capacity + slot_ids, buf_rows)
        src_copy = jnp.full((buf_rows + 1,), copy_count, jnp.int32).at[dest_row.reshape(-1)].set(jnp.arange(copy_count, dtype=jnp.int32))[:buf_rows]
        src_tok = jnp.minimum(src_copy // top_k, tok_local - 1)

        src_slots = src_tok.reshape(experts, capacity)
        x_parts = []
        for lo, hi in zip(x_cuts[:-1], x_cuts[1:]):
            idx = src_slots[:, lo:hi].reshape(-1)
            if x_parts:
                idx, _ = lax.optimization_barrier((idx, x_rows))
            x_rows = jnp.take(hidden, idx, axis=0, mode='clip')
            x_parts.append(lax.all_to_all(x_rows.reshape(experts, hi - lo, d_model), 'ep', 0, 0, tiled=True))

        logits = jnp.dot(hidden, w_router, preferred_element_type=F32) + b_router
        expert_range = jnp.arange(experts, dtype=jnp.int32)
        picked = [expert_ids[:, k:k + 1] == expert_range for k in range(top_k)]
        chosen = jnp.stack([jnp.sum(jnp.where(p, logits, 0.0), axis=1) for p in picked], axis=1)
        gate_w = jax.nn.softmax(chosen, axis=-1)

        row_gate = jnp.zeros((buf_rows + 1,), F32).at[dest_row.reshape(-1)].set(gate_w.reshape(-1))[:buf_rows]
        row_grad = jnp.take(grad_out, src_tok, axis=0, mode='clip')
        send_q = (row_gate[:, None] * row_grad.astype(F32)).astype(BF16)

        col = jnp.arange(2 * ffp, dtype=jnp.int32)
        old_col = jnp.where(col < ffp, 2 * col, 2 * (col - ffp) + 1)
        old_col = jnp.where((col % ffp) < ff, old_col, -1)
        pick = (jnp.arange(ff2, dtype=jnp.int32)[:, None] == old_col[None, :]).astype(BF16)
        w_in = jnp.dot(w_gate_up[0], pick, preferred_element_type=F32).astype(BF16)
        b_pair = b_gate_up[0].reshape(ff, 2)
        b_in = jnp.concatenate([jnp.pad(b_pair[:, 0], (0, ffp - ff)), jnp.pad(b_pair[:, 1], (0, ffp - ff))])
        w_out = jnp.pad(w_down[0], ((0, ffp - ff), (0, 0)))

        *x_parts, send_q = lax.optimization_barrier((*x_parts, send_q))
        recv_q = lax.all_to_all(send_q, 'ep', 0, 0, tiled=True)
        recv_x = jnp.concatenate(x_parts, axis=1).reshape(buf_rows, d_model)

        pre_act = jnp.dot(recv_x, w_in, preferred_element_type=F32) + b_in
        act_val, act_vjp = jax.vjp(swiglu, pre_act[:, :ffp], pre_act[:, ffp:])
        act_bf = act_val.astype(BF16)
        y_rows = (jnp.dot(act_bf, w_out, preferred_element_type=F32) + b_down[0]).astype(BF16)
        recv_q, y_rows = lax.optimization_barrier((recv_q, y_rows))
        back_y = lax.all_to_all(y_rows, 'ep', 0, 0, tiled=True)

        act_grad = lax.dot_general(recv_q, w_out, COLS_LAST, preferred_element_type=F32)
        gate_pre, up_pre = act_vjp(act_grad)
        pre_grad_in = jnp.concatenate([gate_pre.astype(BF16), up_pre.astype(BF16)], axis=1)
        p_sends = [lax.dot_general(pre_grad_in, w_in[lo:hi], COLS_LAST, preferred_element_type=F32).astype(BF16) for lo, hi in zip(p_cuts[:-1], p_cuts[1:])]
        pre_grad = lax.dot_general(pre_grad_in, pick, COLS_LAST, preferred_element_type=F32).astype(BF16)
        grad_b_down = jnp.sum(recv_q, axis=0, dtype=F32)
        grad_b_gate_up = jnp.sum(pre_grad, axis=0, dtype=F32)
        grad_w_down = lax.dot_general(act_bf, recv_q, ROWS_FIRST, preferred_element_type=F32)[:ff]
        back_y, p_sends[0], grad_w_down, grad_b_down, pre_grad = lax.optimization_barrier((back_y, p_sends[0], grad_w_down, grad_b_down, pre_grad))
        p_first = lax.all_to_all(p_sends[0], 'ep', 0, 0, tiled=True)
        grad_w_gate_up = lax.dot_general(recv_x, pre_grad, ROWS_FIRST, preferred_element_type=F32)

        def copies_of(buf):
            return [jnp.take(buf, jnp.minimum(dest_row[:, k], buf_rows - 1), axis=0, mode='clip') for k in range(top_k)]

        y_copies = [jnp.where(kept[:, k:k + 1], rows.astype(F32), 0.0) for k, rows in enumerate(copies_of(back_y))]
        block_out = sum(gate_w[:, k:k + 1] * y_copies[k] for k in range(top_k)).astype(BF16)
        gate_grad = jnp.stack([jnp.sum(grad_out.astype(F32) * y, axis=1) for y in y_copies], axis=1)
        sel_grad = gate_w * (gate_grad - jnp.sum(gate_w * gate_grad, axis=1, keepdims=True))
        logit_grad = sum(jnp.where(picked[k], sel_grad[:, k:k + 1], 0.0) for k in range(top_k)).astype(BF16)

        router_part = lax.dot_general(logit_grad, hidden, ROWS_FIRST, preferred_element_type=F32)
        bias_part = jnp.sum(logit_grad, axis=0, dtype=F32)
        part = jnp.concatenate([router_part, jnp.broadcast_to(bias_part[:, None], (experts, 128))], axis=1)
        total = jnp.sum(lax.all_gather(part, 'ep'), axis=0)
        grad_w_router = total[:, :d_model].T
        grad_b_router = total[:, d_model]

        p_first, p_sends[1], block_out, logit_grad, grad_w_gate_up = lax.optimization_barrier((p_first, p_sends[1], block_out, logit_grad, grad_w_gate_up))
        p_last = lax.all_to_all(p_sends[1], 'ep', 0, 0, tiled=True)

        keep = kept.astype(F32)
        router_t = w_router.T
        grad_hidden = None
        for lo, buf in zip(p_cuts, (p_first, p_last)):
            grad_hidden = add_copies(*copies_of(buf), keep, logit_grad, router_t, lo, grad_hidden)
        return (block_out, grad_hidden, grad_w_router, grad_b_router, grad_w_gate_up[None], grad_b_gate_up[None], grad_w_down[None], grad_b_down[None])

    tok_spec = P('ep', None)
    in_specs = (tok_spec, tok_spec, P(None, None), P(None), tok_spec, tok_spec, P('ep', None, None), P('ep', None), P('ep', None, None), P('ep', None))
    out_specs = (tok_spec, tok_spec, P(None, None), P(None), P('ep', None, None), P('ep', None), P('ep', None, None), P('ep', None))
    return jax.shard_map(block, mesh=mesh, in_specs=in_specs, out_specs=out_specs, check_vma=False)
```

```python
import jax
import jax.numpy as jnp
import numpy as np
from jax import lax
from jax.experimental import pallas as pl
from jax.sharding import PartitionSpec as P

SWIGLU_LIMIT = 7.0
SWIGLU_ALPHA = 1.702
F32 = jnp.float32
BF16 = jnp.bfloat16
ROWS_FIRST = (((0,), (0,)), ((), ()))
COLS_LAST = (((1,), (1,)), ((), ()))


def swiglu(gate, up):
    gate_in = jnp.minimum(gate, SWIGLU_LIMIT)
    up_in = jnp.clip(up, -SWIGLU_LIMIT, SWIGLU_LIMIT)
    return gate_in * jax.nn.sigmoid(SWIGLU_ALPHA * gate_in) * (up_in + 1.0)


def round_up(value, unit):
    return (value + unit - 1) // unit * unit


def add_copies_kernel(first_ref, second_ref, keep_ref, logit_ref, router_ref, *refs):
    out_ref = refs[-1]
    keep = keep_ref[...]
    total = jnp.where(keep[:, 0:1] > 0, first_ref[...].astype(F32), 0.0) + jnp.where(keep[:, 1:2] > 0, second_ref[...].astype(F32), 0.0)
    total += jnp.dot(logit_ref[...], router_ref[...], preferred_element_type=F32)
    out_ref[...] = total.astype(BF16)


def add_copies(first, second, keep, logit_grad, router_t, lo, into):
    rows, cols = first.shape
    d_model = router_t.shape[1]
    experts = router_t.shape[0]
    tm, tn = min(rows, 512), min(cols, 1024)
    base = lo // tn
    args = [first, second, keep, logit_grad, router_t]
    specs = [
        pl.BlockSpec((tm, tn), lambda i, j: (i, j)),
        pl.BlockSpec((tm, tn), lambda i, j: (i, j)),
        pl.BlockSpec((tm, 2), lambda i, j: (i, 0)),
        pl.BlockSpec((tm, experts), lambda i, j: (i, 0)),
        pl.BlockSpec((experts, tn), lambda i, j: (0, j + base)),
    ]
    aliases = {}
    if into is not None:
        args.append(into)
        specs.append(pl.BlockSpec(memory_space=pl.ANY))
        aliases = {5: 0}
    return pl.pallas_call(
        add_copies_kernel,
        out_shape=jax.ShapeDtypeStruct((rows, d_model), BF16),
        grid=(rows // tm, cols // tn),
        in_specs=specs,
        out_specs=pl.BlockSpec((tm, tn), lambda i, j: (i, j + base)),
        input_output_aliases=aliases,
        cost_estimate=pl.CostEstimate(flops=20 * rows * cols, bytes_accessed=6 * rows * cols, transcendentals=0),
    )(*args)


def solution(mesh):
    ep_size = mesh.shape['ep']

    def block(hidden, grad_out, w_router, b_router, expert_ids, slot_ids, w_gate_up, b_gate_up, w_down, b_down):
        tok_local, d_model = hidden.shape
        top_k = expert_ids.shape[1]
        experts = w_router.shape[1]
        ff2 = w_gate_up.shape[2]
        ff = ff2 // 2
        ffp = round_up(ff, 128)
        capacity = (3 * tok_local * top_k + 2 * experts - 1) // (2 * experts)
        buf_rows = experts * capacity
        x_cuts = (0, round_up(capacity // 6, 8), capacity)
        p_cuts = (0, d_model * 3 // 4, d_model)

        kept = slot_ids >= 0
        expert_range = jnp.arange(experts, dtype=jnp.int32)
        picked = [expert_ids[:, k:k + 1] == expert_range for k in range(top_k)]
        token = np.arange(tok_local, dtype=np.int32)
        src_copy = 0
        for k in range(top_k):
            number = (jnp.arange(tok_local, dtype=jnp.int32) * top_k + (k + 1))[:, None]
            digits = jnp.concatenate([jnp.where(picked[k], number >> 6, 0), jnp.where(picked[k], number & 63, 0)], axis=1).astype(BF16)
            in_slot = (slot_ids[:, k:k + 1] == jnp.arange(capacity, dtype=jnp.int32)).astype(BF16)
            src_copy += lax.dot_general(digits, in_slot, ROWS_FIRST, preferred_element_type=F32)
        src_copy = (src_copy[:experts] * 64.0 + src_copy[experts:]).astype(jnp.int32)
        spread = (np.arange(buf_rows, dtype=np.int32) % tok_local).reshape(experts, capacity)
        src_slots = jnp.where(src_copy > 0, (src_copy - 1) // top_k, spread)
        dest_row = expert_ids * capacity + jnp.where(kept, slot_ids, (token % capacity)[:, None])

        x_parts = []
        for lo, hi in zip(x_cuts[:-1], x_cuts[1:]):
            idx = src_slots[:, lo:hi].reshape(-1)
            if x_parts:
                idx, _ = lax.optimization_barrier((idx, x_rows))
            x_rows = jnp.take(hidden, idx, axis=0, mode='clip')
            x_parts.append(lax.all_to_all(x_rows.reshape(experts, hi - lo, d_model), 'ep', 0, 0, tiled=True))

        logits = jnp.dot(hidden, w_router, preferred_element_type=F32) + b_router
        chosen = jnp.stack([jnp.sum(jnp.where(p, logits, 0.0), axis=1) for p in picked], axis=1)
        gate_w = jax.nn.softmax(chosen, axis=-1)

        gate_row = jnp.where(kept, dest_row, buf_rows)
        row_gate = jnp.zeros((buf_rows + 1,), F32).at[gate_row.reshape(-1)].set(gate_w.reshape(-1))[:buf_rows]
        row_grad = jnp.take(grad_out, src_slots.reshape(-1), axis=0, mode='clip')
        send_q = (row_gate[:, None] * row_grad.astype(F32)).astype(BF16)

        col = jnp.arange(2 * ffp, dtype=jnp.int32)
        old_col = jnp.where(col < ffp, 2 * col, 2 * (col - ffp) + 1)
        old_col = jnp.where((col % ffp) < ff, old_col, -1)
        pick = (jnp.arange(ff2, dtype=jnp.int32)[:, None] == old_col[None, :]).astype(BF16)
        w_in = jnp.dot(w_gate_up[0], pick, preferred_element_type=F32).astype(BF16)
        b_pair = b_gate_up[0].reshape(ff, 2)
        b_in = jnp.concatenate([jnp.pad(b_pair[:, 0], (0, ffp - ff)), jnp.pad(b_pair[:, 1], (0, ffp - ff))])
        w_out = jnp.pad(w_down[0], ((0, ffp - ff), (0, 0)))

        *x_parts, send_q = lax.optimization_barrier((*x_parts, send_q))
        recv_q = lax.all_to_all(send_q, 'ep', 0, 0, tiled=True)
        recv_x = jnp.concatenate(x_parts, axis=1).reshape(buf_rows, d_model)

        pre_act = jnp.dot(recv_x, w_in, preferred_element_type=F32) + b_in
        act_val, act_vjp = jax.vjp(swiglu, pre_act[:, :ffp], pre_act[:, ffp:])
        act_bf = act_val.astype(BF16)
        y_rows = (jnp.dot(act_bf, w_out, preferred_element_type=F32) + b_down[0]).astype(BF16)
        recv_q, y_rows = lax.optimization_barrier((recv_q, y_rows))
        back_y = lax.all_to_all(y_rows, 'ep', 0, 0, tiled=True)

        act_grad = lax.dot_general(recv_q, w_out, COLS_LAST, preferred_element_type=F32)
        gate_pre, up_pre = act_vjp(act_grad)
        pre_grad_in = jnp.concatenate([gate_pre.astype(BF16), up_pre.astype(BF16)], axis=1)
        p_sends = [lax.dot_general(pre_grad_in, w_in[lo:hi], COLS_LAST, preferred_element_type=F32).astype(BF16) for lo, hi in zip(p_cuts[:-1], p_cuts[1:])]
        pre_grad = lax.dot_general(pre_grad_in, pick, COLS_LAST, preferred_element_type=F32).astype(BF16)
        grad_b_down = jnp.sum(recv_q, axis=0, dtype=F32)
        grad_w_down = lax.dot_general(act_bf, recv_q, ROWS_FIRST, preferred_element_type=F32)[:ff]
        grad_b_gate_up = jnp.sum(pre_grad, axis=0, dtype=F32)
        back_y, p_sends[0], grad_w_down, grad_b_down, pre_grad = lax.optimization_barrier((back_y, p_sends[0], grad_w_down, grad_b_down, pre_grad))
        p_first = lax.all_to_all(p_sends[0], 'ep', 0, 0, tiled=True)
        grad_w_gate_up = lax.dot_general(recv_x, pre_grad, ROWS_FIRST, preferred_element_type=F32)

        def copies_of(buf):
            return [jnp.take(buf, dest_row[:, k], axis=0, mode='clip') for k in range(top_k)]

        y_copies = [jnp.where(kept[:, k:k + 1], rows.astype(F32), 0.0) for k, rows in enumerate(copies_of(back_y))]
        block_out = sum(gate_w[:, k:k + 1] * y_copies[k] for k in range(top_k)).astype(BF16)
        gate_grad = jnp.stack([jnp.sum(grad_out.astype(F32) * y, axis=1) for y in y_copies], axis=1)
        sel_grad = gate_w * (gate_grad - jnp.sum(gate_w * gate_grad, axis=1, keepdims=True))
        logit_grad = sum(jnp.where(picked[k], sel_grad[:, k:k + 1], 0.0) for k in range(top_k)).astype(BF16)

        piece = d_model // ep_size
        router_part = lax.dot_general(logit_grad, hidden, ROWS_FIRST, preferred_element_type=F32)
        bias_part = jnp.sum(logit_grad, axis=0, dtype=F32)
        part = jnp.concatenate([router_part.reshape(experts, ep_size, piece).swapaxes(0, 1), jnp.broadcast_to(bias_part[None, :, None], (ep_size, experts, 128))], axis=2)

        p_first, p_sends[1], block_out, logit_grad, grad_w_gate_up, part = lax.optimization_barrier((p_first, p_sends[1], block_out, logit_grad, grad_w_gate_up, part))
        p_last = lax.all_to_all(p_sends[1], 'ep', 0, 0, tiled=True)

        part = lax.all_to_all(part, 'ep', 0, 0, tiled=True)
        mine = jnp.sum(part, axis=0)
        pieces = lax.all_to_all(jnp.broadcast_to(mine, (ep_size, experts, piece + 128)), 'ep', 0, 0, tiled=True)
        grad_w_router = pieces[:, :, :piece].swapaxes(0, 1).reshape(experts, d_model).T
        grad_b_router = pieces[0, :, piece]

        keep = kept.astype(F32)
        router_t = w_router.T
        grad_hidden = add_copies(*copies_of(p_first), keep, logit_grad, router_t, p_cuts[0], None)
        last_copies = copies_of(p_last)
        grad_hidden = add_copies(*last_copies, keep, logit_grad, router_t, p_cuts[1], grad_hidden)
        return (block_out, grad_hidden, grad_w_router, grad_b_router, grad_w_gate_up[None], grad_b_gate_up[None], grad_w_down[None], grad_b_down[None])

    tok_spec = P('ep', None)
    in_specs = (tok_spec, tok_spec, P(None, None), P(None), tok_spec, tok_spec, P('ep', None, None), P('ep', None), P('ep', None, None), P('ep', None))
    out_specs = (tok_spec, tok_spec, P(None, None), P(None), P('ep', None, None), P('ep', None), P('ep', None, None), P('ep', None))
    return jax.shard_map(block, mesh=mesh, in_specs=in_specs, out_specs=out_specs, check_vma=False)
```

```python
import jax
import jax.numpy as jnp
import numpy as np
from jax import lax
from jax.experimental import pallas as pl
from jax.experimental.pallas import tpu as pltpu
from jax.sharding import PartitionSpec as P

SWIGLU_LIMIT = 7.0
SWIGLU_ALPHA = 1.702
F32 = jnp.float32
BF16 = jnp.bfloat16
ROWS_FIRST = (((0,), (0,)), ((), ()))
COLS_LAST = (((1,), (1,)), ((), ()))


def swiglu(gate, up):
    gate_in = jnp.minimum(gate, SWIGLU_LIMIT)
    up_in = jnp.clip(up, -SWIGLU_LIMIT, SWIGLU_LIMIT)
    return gate_in * jax.nn.sigmoid(SWIGLU_ALPHA * gate_in) * (up_in + 1.0)


def round_up(value, unit):
    return (value + unit - 1) // unit * unit


def add_copies_kernel(first_ref, second_ref, keep_ref, logit_ref, router_ref, *refs):
    out_ref = refs[-1]
    keep = keep_ref[...]
    total = jnp.where(keep[:, 0:1] > 0, first_ref[...].astype(F32), 0.0) + jnp.where(keep[:, 1:2] > 0, second_ref[...].astype(F32), 0.0)
    total += jnp.dot(logit_ref[...], router_ref[...], preferred_element_type=F32)
    out_ref[...] = total.astype(BF16)


def add_copies(first, second, keep, logit_grad, router_t, lo, into):
    rows, cols = first.shape
    d_model = router_t.shape[1]
    experts = router_t.shape[0]
    tm, tn = min(rows, 512), min(cols, 1024)
    base = lo // tn
    args = [first, second, keep, logit_grad, router_t]
    specs = [
        pl.BlockSpec((tm, tn), lambda i, j: (i, j)),
        pl.BlockSpec((tm, tn), lambda i, j: (i, j)),
        pl.BlockSpec((tm, 2), lambda i, j: (i, 0)),
        pl.BlockSpec((tm, experts), lambda i, j: (i, 0)),
        pl.BlockSpec((experts, tn), lambda i, j: (0, j + base)),
    ]
    aliases = {}
    if into is not None:
        args.append(into)
        specs.append(pl.BlockSpec(memory_space=pl.ANY))
        aliases = {5: 0}
    return pl.pallas_call(
        add_copies_kernel,
        out_shape=jax.ShapeDtypeStruct((rows, d_model), BF16),
        grid=(rows // tm, cols // tn),
        in_specs=specs,
        out_specs=pl.BlockSpec((tm, tn), lambda i, j: (i, j + base)),
        input_output_aliases=aliases,
        cost_estimate=pl.CostEstimate(flops=20 * rows * cols, bytes_accessed=6 * rows * cols, transcendentals=0),
    )(*args)


def place_rows_kernel(owners, halves, me_ref, *refs):
    count = len(owners)
    pieces, out_ref, buf, in_sem, out_sem = refs[:count], refs[count], refs[count + 1], refs[count + 2], refs[count + 3]
    slots, lag = buf.shape[0], 2
    cols = buf.shape[2]
    me = me_ref[0]
    ins = [pltpu.make_async_copy(pieces[i], buf.at[i % slots], in_sem.at[i % slots]) for i in range(count)]
    outs = [
        pltpu.make_async_copy(buf.at[i % slots], out_ref.at[me ^ owners[i], :, pl.ds(halves[i] * cols, cols)], out_sem.at[i % slots])
        for i in range(count)
    ]
    for i in range(count + lag):
        if i < count:
            if i >= slots:
                outs[i - slots].wait()
            ins[i].start()
        if i >= lag:
            ins[i - lag].wait()
            outs[i - lag].start()
    for copy in outs[-slots:]:
        copy.wait()


def place_rows(pieces, owners, halves, me, ep_size):
    rows, cols = pieces[0].shape
    slots = 6
    return pl.pallas_call(
        lambda *refs: place_rows_kernel(owners, halves, *refs),
        out_shape=jax.ShapeDtypeStruct((ep_size, rows, 2 * cols), BF16),
        in_specs=[pl.BlockSpec(memory_space=pltpu.SMEM)] + [pl.BlockSpec(memory_space=pl.ANY)] * len(pieces),
        out_specs=pl.BlockSpec(memory_space=pl.ANY),
        scratch_shapes=[pltpu.VMEM((slots, rows, cols), BF16), pltpu.SemaphoreType.DMA((slots,)), pltpu.SemaphoreType.DMA((slots,))],
        compiler_params=pltpu.CompilerParams(vmem_limit_bytes=slots * rows * cols * 2 + (1 << 20)),
        cost_estimate=pl.CostEstimate(flops=200_000_000, bytes_accessed=4 * ep_size * rows * 2 * cols, transcendentals=0),
        name='place_rows',
    )(me.reshape(1), *pieces)


def solution(mesh):
    ep_size = mesh.shape['ep']

    def block(hidden, grad_out, w_router, b_router, expert_ids, slot_ids, w_gate_up, b_gate_up, w_down, b_down):
        tok_local, d_model = hidden.shape
        top_k = expert_ids.shape[1]
        experts = w_router.shape[1]
        ff2 = w_gate_up.shape[2]
        ff = ff2 // 2
        ffp = round_up(ff, 128)
        capacity = (3 * tok_local * top_k + 2 * experts - 1) // (2 * experts)
        buf_rows = experts * capacity
        p_cuts = (0, d_model * 3 // 4, d_model)

        half = d_model // 2
        me = lax.axis_index('ep')

        def shift(value, mask):
            return lax.ppermute(value, 'ep', [(d, d ^ mask) for d in range(ep_size)])

        across = (2, 4)
        targets = ((1, 4, 5, 0), (1, 2, 3, 0))
        halves_of = lambda array: (array[:, :half], array[:, half:])
        hidden_halves = halves_of(hidden)
        hidden_near = [shift(v, m) for v, m in zip(hidden_halves, across)]
        ids = jnp.concatenate([expert_ids.T, slot_ids.T], axis=0)
        near_ids = [shift(ids, m) for m in across]

        kept = slot_ids >= 0
        expert_range = jnp.arange(experts, dtype=jnp.int32)
        picked = [expert_ids[:, k:k + 1] == expert_range for k in range(top_k)]
        token = np.arange(tok_local, dtype=np.int32)
        spread = (np.arange(buf_rows, dtype=np.int32) % tok_local).reshape(experts, capacity)
        dest_row = expert_ids * capacity + jnp.where(kept, slot_ids, (token % capacity)[:, None])

        def source_of(owner_ids):
            table = 0
            for k in range(top_k):
                number = (jnp.arange(tok_local, dtype=jnp.int32) * top_k + (k + 1))[None, :]
                hit = (owner_ids[k:k + 1] ^ me) == expert_range[:, None]
                digits = jnp.concatenate([jnp.where(hit, number >> 6, 0), jnp.where(hit, number & 63, 0)], axis=0).astype(BF16)
                in_slot = (owner_ids[top_k + k:top_k + k + 1] == jnp.arange(capacity, dtype=jnp.int32)[:, None]).astype(BF16)
                table += lax.dot_general(digits, in_slot, COLS_LAST, preferred_element_type=F32)
            table = (table[:experts] * 64.0 + table[experts:]).astype(jnp.int32)
            return jnp.where(table > 0, (table - 1) // top_k, spread)

        def gates_of(owner_ids, gates):
            slots = owner_ids[top_k:]
            rows = jnp.where(slots >= 0, (owner_ids[:top_k] ^ me) * capacity + slots, buf_rows)
            return jnp.zeros((buf_rows + 1,), F32).at[rows.reshape(-1)].set(gates.reshape(-1))[:buf_rows].reshape(experts, capacity)

        own_source = source_of(ids)
        near_source = [source_of(i) for i in near_ids]

        def rows_for(h, values, source, gates):
            got = []
            for m in targets[h]:
                rows = jnp.take(values, source[m], axis=0, mode='clip')
                if gates is not None:
                    rows = (gates[m][:, None] * rows.astype(F32)).astype(BF16)
                if m:
                    rows = shift(rows, m)
                got.append(rows)
            return got

        def dispatch(own_values, near_values, own_gates, near_gates):
            pieces, owners, halves = [], [], []
            for h in range(2):
                pieces += rows_for(h, own_values[h], own_source, own_gates)
                owners += targets[h]
                halves += [h] * len(targets[h])
            for h in range(2):
                pieces += rows_for(h, near_values[h], near_source[h], near_gates and near_gates[h])
                owners += [m ^ across[h] for m in targets[h]]
                halves += [h] * len(targets[h])
            return place_rows(pieces, owners, halves, me, ep_size).reshape(buf_rows, d_model)

        recv_x = dispatch(hidden_halves, hidden_near, None, None)

        logits = jnp.dot(hidden, w_router, preferred_element_type=F32) + b_router
        chosen = jnp.stack([jnp.sum(jnp.where(p, logits, 0.0), axis=1) for p in picked], axis=1)
        gate_w = jax.nn.softmax(chosen, axis=-1)
        gate_t = gate_w.T
        near_gate_t = [shift(gate_t, m) for m in across]
        own_gates = gates_of(ids, gate_t)
        near_gates = [gates_of(i, g) for i, g in zip(near_ids, near_gate_t)]
        grad_halves = halves_of(grad_out)
        grad_near = [shift(v, m) for v, m in zip(grad_halves, across)]
        recv_q = dispatch(grad_halves, grad_near, own_gates, near_gates)

        col = jnp.arange(2 * ffp, dtype=jnp.int32)
        old_col = jnp.where(col < ffp, 2 * col, 2 * (col - ffp) + 1)
        old_col = jnp.where((col % ffp) < ff, old_col, -1)
        pick = (jnp.arange(ff2, dtype=jnp.int32)[:, None] == old_col[None, :]).astype(BF16)
        w_in = jnp.dot(w_gate_up[0], pick, preferred_element_type=F32).astype(BF16)
        b_pair = b_gate_up[0].reshape(ff, 2)
        b_in = jnp.concatenate([jnp.pad(b_pair[:, 0], (0, ffp - ff)), jnp.pad(b_pair[:, 1], (0, ffp - ff))])
        w_out = jnp.pad(w_down[0], ((0, ffp - ff), (0, 0)))

        pre_act = jnp.dot(recv_x, w_in, preferred_element_type=F32) + b_in
        act_bf = swiglu(pre_act[:, :ffp], pre_act[:, ffp:]).astype(BF16)
        y_rows = (jnp.dot(act_bf, w_out, preferred_element_type=F32) + b_down[0]).astype(BF16)
        back_y = lax.all_to_all(y_rows, 'ep', 0, 0, tiled=True)

        recv_q, pre_act = lax.optimization_barrier((recv_q, pre_act))
        _, act_vjp = jax.vjp(swiglu, pre_act[:, :ffp], pre_act[:, ffp:])
        act_grad = lax.dot_general(recv_q, w_out, COLS_LAST, preferred_element_type=F32)
        gate_pre, up_pre = act_vjp(act_grad)
        pre_grad_in = jnp.concatenate([gate_pre.astype(BF16), up_pre.astype(BF16)], axis=1)
        p_sends = [lax.dot_general(pre_grad_in, w_in[lo:hi], COLS_LAST, preferred_element_type=F32).astype(BF16) for lo, hi in zip(p_cuts[:-1], p_cuts[1:])]
        pre_grad = lax.dot_general(pre_grad_in, pick, COLS_LAST, preferred_element_type=F32).astype(BF16)
        grad_b_down = jnp.sum(recv_q, axis=0, dtype=F32)
        grad_w_down = lax.dot_general(act_bf, recv_q, ROWS_FIRST, preferred_element_type=F32)[:ff]
        grad_b_gate_up = jnp.sum(pre_grad, axis=0, dtype=F32)
        back_y, p_sends[0], grad_w_down, grad_b_down, pre_grad = lax.optimization_barrier((back_y, p_sends[0], grad_w_down, grad_b_down, pre_grad))
        p_first = lax.all_to_all(p_sends[0], 'ep', 0, 0, tiled=True)
        grad_w_gate_up = lax.dot_general(recv_x, pre_grad, ROWS_FIRST, preferred_element_type=F32)

        def copies_of(buf):
            return [jnp.take(buf, dest_row[:, k], axis=0, mode='clip') for k in range(top_k)]

        y_copies = [jnp.where(kept[:, k:k + 1], rows.astype(F32), 0.0) for k, rows in enumerate(copies_of(back_y))]
        block_out = sum(gate_w[:, k:k + 1] * y_copies[k] for k in range(top_k)).astype(BF16)
        gate_grad = jnp.stack([jnp.sum(grad_out.astype(F32) * y, axis=1) for y in y_copies], axis=1)
        sel_grad = gate_w * (gate_grad - jnp.sum(gate_w * gate_grad, axis=1, keepdims=True))
        logit_grad = sum(jnp.where(picked[k], sel_grad[:, k:k + 1], 0.0) for k in range(top_k)).astype(BF16)

        piece = d_model // ep_size
        router_part = lax.dot_general(logit_grad, hidden, ROWS_FIRST, preferred_element_type=F32)
        bias_part = jnp.sum(logit_grad, axis=0, dtype=F32)
        part = jnp.concatenate([router_part.reshape(experts, ep_size, piece).swapaxes(0, 1), jnp.broadcast_to(bias_part[None, :, None], (ep_size, experts, 128))], axis=2)

        p_first, p_sends[1], block_out, logit_grad, grad_w_gate_up, part = lax.optimization_barrier((p_first, p_sends[1], block_out, logit_grad, grad_w_gate_up, part))
        p_last = lax.all_to_all(p_sends[1], 'ep', 0, 0, tiled=True)

        part = lax.all_to_all(part, 'ep', 0, 0, tiled=True)
        mine = jnp.sum(part, axis=0)
        pieces = lax.all_to_all(jnp.broadcast_to(mine, (ep_size, experts, piece + 128)), 'ep', 0, 0, tiled=True)
        grad_w_router = pieces[:, :, :piece].swapaxes(0, 1).reshape(experts, d_model).T
        grad_b_router = pieces[0, :, piece]

        keep = kept.astype(F32)
        router_t = w_router.T
        grad_hidden = add_copies(*copies_of(p_first), keep, logit_grad, router_t, p_cuts[0], None)
        last_copies = copies_of(p_last)
        grad_hidden = add_copies(*last_copies, keep, logit_grad, router_t, p_cuts[1], grad_hidden)
        return (block_out, grad_hidden, grad_w_router, grad_b_router, grad_w_gate_up[None], grad_b_gate_up[None], grad_w_down[None], grad_b_down[None])

    tok_spec = P('ep', None)
    in_specs = (tok_spec, tok_spec, P(None, None), P(None), tok_spec, tok_spec, P('ep', None, None), P('ep', None), P('ep', None, None), P('ep', None))
    out_specs = (tok_spec, tok_spec, P(None, None), P(None), P('ep', None, None), P('ep', None), P('ep', None, None), P('ep', None))
    return jax.shard_map(block, mesh=mesh, in_specs=in_specs, out_specs=out_specs, check_vma=False)
```
